8 devices in a mesh: dp: 2 (over y, z), sp: 4 (over x, core).
Axes of the slice: x: 2, y: 2, z: 1, core: 2. Of those that a mesh axis runs over, the one named last changes fastest.
Arguments:
- x: bfloat16 [4096, 2048], P(('dp', 'sp')), parts along dimension 0
- gain: bfloat16 [2048], replicated
- wq: bfloat16 [2048, 2048], replicated
- wk: bfloat16 [2048, 2048], replicated
- wv: bfloat16 [2048, 2048], replicated
- wo: bfloat16 [2048, 2048], replicated
Outputs:
- output: bfloat16 [4096, 2048], P(('dp', 'sp')), parts along dimension 0
There are 2 independent parts. The reference program is written for one: setup_inputs(seed, part) draws one part's arguments, and reference() takes and returns one part's arrays. A program takes and returns all parts, laid end to end along the dimension named above; an argument that names none is the same for every part.
All inputs are finite; a program needn't handle non-finite values.
Results may differ from the reference program's by a relative error of at most 0.012.
Values are sent between devices in bfloat16 or wider.
A program may use at most 2 GiB of HBM per device.

```python
import jax
import jax.numpy as jnp
from jax import lax

ROWS = 2048
D = 2048
HEADS = 16
KV_HEADS = 16
HEAD = 128
THETA = 10000


def setup_inputs(seed: int = 0, part: int = 0) -> dict:
    kx, kn, kq, kk, kv, ko = jax.random.split(jax.random.key(seed), 6)

    def weights(key, rows, columns):
        return jax.random.normal(key, (rows, columns), jnp.float32) * rows**-0.5

    drawn = {
        "x": jax.random.normal(jax.random.fold_in(kx, part), (ROWS, D), jnp.float32),
        "gain": 1 + 0.1 * jax.random.normal(kn, (D,), jnp.float32),
        "wq": 2 * weights(kq, D, HEADS * HEAD),
        "wk": 2 * weights(kk, D, KV_HEADS * HEAD),
        "wv": 4 * weights(kv, D, KV_HEADS * HEAD),
        "wo": weights(ko, HEADS * HEAD, D),
    }
    return {k: v.astype(jnp.bfloat16) for k, v in drawn.items()}


def normed(x, gain):
    wide = x.astype(jnp.float32)
    scale = lax.rsqrt(jnp.mean(wide * wide, -1, keepdims=True) + 1e-6)
    return (wide * scale * gain.astype(jnp.float32)).astype(jnp.bfloat16)


def turned(t, place, theta):
    half = t.shape[-1] // 2
    angle = place.astype(jnp.float32)[:, None] * theta ** (-jnp.arange(half, dtype=jnp.float32) / half)
    cos, sin = jnp.cos(angle)[:, None], jnp.sin(angle)[:, None]
    a, b = t[..., :half].astype(jnp.float32), t[..., half:].astype(jnp.float32)
    return jnp.concatenate([a * cos - b * sin, b * cos + a * sin], -1).astype(jnp.bfloat16)


def matmul(a, w):
    return jnp.dot(a, w, preferred_element_type=jnp.float32).astype(jnp.bfloat16)


def einsum(form, a, b):
    return jnp.einsum(form, a.astype(jnp.float32), b.astype(jnp.float32))


def attention(q, k, v):
    scores = einsum("tgsd,ugd->gstu", q, k) * q.shape[-1] ** -0.5
    token = jnp.arange(q.shape[0])
    scores = jnp.where(token[:, None] >= token, scores, -jnp.inf)
    weights = jax.nn.softmax(scores, -1).astype(jnp.bfloat16)
    return einsum("gstu,ugd->tgsd", weights, v).astype(jnp.bfloat16)


def reference(x, gain, wq, wk, wv, wo):
    a, place = normed(x, gain), jnp.arange(ROWS)
    q = turned(matmul(a, wq).reshape(ROWS, HEADS, HEAD), place, THETA).reshape(ROWS, KV_HEADS, -1, HEAD)
    k = turned(matmul(a, wk).reshape(ROWS, KV_HEADS, HEAD), place, THETA)
    v = matmul(a, wv).reshape(ROWS, KV_HEADS, HEAD)
    seen = attention(q, k, v).reshape(ROWS, HEADS * HEAD)
    return (x.astype(jnp.float32) + jnp.dot(seen, wo, preferred_element_type=jnp.float32)).astype(jnp.bfloat16)
```

```python
import functools

import jax
import jax.numpy as jnp
import numpy as np
from jax import lax
from jax.experimental import pallas as pl
from jax.experimental.pallas import tpu as pltpu
from jax.sharding import PartitionSpec as P

HEAD = 128
THETA = 10000
D = 2048
OWN = 512
CHIP = 1024
HEADS = 8
WIDE = HEADS * HEAD
TILE = 256
TILES = WIDE // TILE
UNITS = 4
UNIT = CHIP // UNITS
PART = UNIT // 2
HIDDEN = -2e30
LOG2E = 1.4426950408889634
SCALE = HEAD**-0.5 * LOG2E
VROWS = HEAD + 16
MESH = pl.DeviceIdType.MESH
F32, BF16 = jnp.float32, jnp.bfloat16


def rope_table():
    half = HEAD // 2
    place = np.arange(2 * CHIP, dtype=np.float32)[:, None]
    angle = place * np.power(np.float32(THETA), -np.arange(half, dtype=np.float32) / np.float32(half)).astype(np.float32)
    return np.concatenate([np.cos(angle), np.sin(angle)], -1).astype(np.float32)


def dot(a, b, ca=1, cb=0):
    return lax.dot_general(a, b, (((ca,), (cb,)), ((), ())), preferred_element_type=F32)


def kernel(x_ref, gain_ref, wq_ref, wk_ref, wv_ref, wo_ref, rope_ref, y_ref,
           xs, x0, a_s, w_s, wo_s, q_s, k_s, v_s, k0_s, v0_s, cos_s, sin_s, rope_s, top_s, mix_s, og_s, os_s, yacc_s, y_s,
           x_sem, w_sem, wo_sem, rope_sem, pair_sem, link_send, link_recv, fwd_send, fwd_recv, o_send, o_recv, y_sem):
    me = lax.axis_index("sp")
    chip, core = lax.div(me, 2), lax.rem(me, 2)
    partner, across = 2 * chip + 1 - core, lax.rem(me + 2, 4)

    barrier = pltpu.get_barrier_semaphore()
    for other in (partner, across):
        pl.semaphore_signal(barrier, inc=1, device_id={"sp": other}, device_id_type=MESH)
    pl.semaphore_wait(barrier, 2)

    def link(j):
        return pltpu.make_async_remote_copy(
            src_ref=x_ref.at[pl.ds(j * PART, PART)], dst_ref=x0.at[j, pl.ds(core * PART, PART)], send_sem=link_send.at[j],
            recv_sem=link_recv.at[j], device_id={"sp": across}, device_id_type=MESH)

    def forward(j):
        rows = x0.at[j, pl.ds(core * PART, PART)]
        return pltpu.make_async_remote_copy(src_ref=rows, dst_ref=rows, send_sem=fwd_send.at[j], recv_sem=fwd_recv.at[j],
                                            device_id={"sp": partner}, device_id_type=MESH)

    own_rows = pl.ds(core * OWN, OWN)
    pair = pltpu.make_async_remote_copy(src_ref=x_ref, dst_ref=xs.at[own_rows], send_sem=pair_sem.at[0], recv_sem=pair_sem.at[1],
                                        device_id={"sp": partner}, device_id_type=MESH)
    x_copy = pltpu.make_async_copy(x_ref, xs.at[own_rows], x_sem)
    rope_copy = pltpu.make_async_copy(rope_ref, rope_s, rope_sem)
    wo_copy = pltpu.make_async_copy(wo_ref, wo_s, wo_sem)

    def w_copy(n, which):
        ref = (wq_ref, wk_ref, wv_ref)[which]
        cols = pl.ds(pl.multiple_of(core * WIDE + n * TILE, TILE), TILE)
        return pltpu.make_async_copy(ref.at[:, cols], w_s.at[which, n], w_sem.at[which, n])

    x_copy.start()

    @pl.when(chip == 0)
    def _():
        for j in range(UNITS):
            link(j).start()

    for which in range(3):
        w_copy(0, which).start()
    rope_copy.start()
    pair.start()
    for n in range(1, TILES):
        for which in range(3):
            w_copy(n, which).start()
    wo_copy.start()

    v_s[:, HEAD:, :] = jnp.ones((HEADS, VROWS - HEAD, CHIP), BF16)
    v0_s[:, HEAD:, :] = jnp.ones((HEADS, VROWS - HEAD, UNIT), BF16)

    def norm(get, count):
        def step(i, _):
            wide = get(i).astype(F32)
            scale = lax.rsqrt(jnp.mean(wide * wide, -1, keepdims=True) + 1e-6)
            a_s[pl.ds(i * 64, 64), :] = (wide * scale * gain_ref[...].astype(F32)).astype(BF16)
        lax.fori_loop(0, count // 64, step, None)

    def angles(at, rows, to):
        t = rope_s[pl.ds(at, rows), :]
        r = pltpu.roll(t, 64, 1)
        low = lax.broadcasted_iota(jnp.int32, t.shape, 1) < 64
        cos_s[to : to + rows, :] = jnp.where(low, t, r)
        sin_s[to : to + rows, :] = jnp.where(low, -r, t)

    def turn(t, rows):
        t = t.astype(BF16).astype(F32)
        return (t * cos_s[:rows, :] + pltpu.roll(t, 64, 1) * sin_s[:rows, :]).astype(BF16)

    x_copy.wait()
    rope_copy.wait()

    def project(half, first):
        rows = pl.ds(pl.multiple_of(half * OWN, OWN), OWN)
        norm(lambda i: xs[pl.ds(half * OWN + i * 64, 64), :], OWN)
        angles(pl.multiple_of(chip * CHIP + half * OWN, OWN), OWN, 0)

        def step(n, _):
            if first:
                for which in range(3):
                    w_copy(n, which).wait()
            a = a_s[...]
            q, k, v = (dot(a, w_s[which, n]) for which in range(3))
            for h in range(2):
                cols = slice(h * HEAD, (h + 1) * HEAD)
                q_s[2 * n + h, rows, :] = turn(q[:, cols], OWN)
                k_s[2 * n + h, rows, :] = turn(k[:, cols], OWN)
                v_s[2 * n + h, :HEAD, rows] = v[:, cols].T.astype(BF16)
        lax.fori_loop(0, TILES, step, None)

    project(core, True)
    pair.wait()
    project(1 - core, False)

    def within(h, _):
        for b in range(CHIP // 256):
            cols, seen = slice(b * 256, (b + 1) * 256), (b + 1) * 256
            s = dot(k_s[h, :seen, :], q_s[h, cols, :], 1, 1)
            last = s[seen - 256 :]
            ok = lax.broadcasted_iota(jnp.int32, (256, 256), 1) >= lax.broadcasted_iota(jnp.int32, (256, 256), 0)
            last = jnp.where(ok, last, HIDDEN)
            s = jnp.concatenate([s[: seen - 256], last], 0) if b else last
            top = s.max(0, keepdims=True)
            top_s[h, :, cols] = top
            mix_s[h, :, cols] = dot(v_s[h, :, :seen], jnp.exp2((s - top) * SCALE).astype(BF16))
    lax.fori_loop(0, HEADS, within, None)

    def o_copy(p):
        cols = pl.ds(pl.multiple_of((core * TILES + p) * TILE, TILE), TILE)
        return pltpu.make_async_remote_copy(src_ref=os_s.at[p], dst_ref=og_s.at[:, cols], send_sem=o_send.at[p], recv_sem=o_recv.at[p],
                                            device_id={"sp": partner}, device_id_type=MESH)

    def finish(p, _):
        for h in range(2):
            mix = mix_s.at[2 * p + h]
            for half in range(2):
                cols = slice(half * OWN, (half + 1) * OWN)
                o = (mix[:HEAD, cols] * (1 / mix[HEAD : HEAD + 1, cols])).T.astype(BF16)

                @pl.when(core == half)
                def _():
                    og_s[:, pl.ds(pl.multiple_of((core * TILES + p) * TILE + h * HEAD, HEAD), HEAD)] = o

                @pl.when(core != half)
                def _():
                    os_s[p, :, h * HEAD : (h + 1) * HEAD] = o
        o_copy(p).start()

    @pl.when(chip == 1)
    def _():
        def unit(j, _):
            link(j).wait_recv()
            forward(j).start()
            forward(j).wait_recv()
            norm(lambda i: x0[j, pl.ds(i * 64, 64), :], UNIT)
            for part in range(2):
                angles(pl.multiple_of(part * OWN + j * PART, PART), PART, part * PART)

            def keys(n, _):
                a = a_s[:UNIT, :]
                k, v = (dot(a, w_s[which, n]) for which in (1, 2))
                for h in range(2):
                    cols = slice(h * HEAD, (h + 1) * HEAD)
                    k0_s[2 * n + h] = turn(k[:, cols], UNIT)
                    v0_s[2 * n + h, :HEAD, :] = v[:, cols].T.astype(BF16)
            lax.fori_loop(0, TILES, keys, None)

            def head(h, _):
                strips = [slice(c, c + 512) for c in range(0, CHIP, 512)]
                scores = [dot(k0_s[h], q_s[h, cols, :], 1, 1) for cols in strips]
                for cols, s in zip(strips, scores):
                    old = top_s[h, :, cols]
                    top = jnp.maximum(old, s.max(0, keepdims=True))
                    top_s[h, :, cols] = top
                    p = jnp.exp2((s - top) * SCALE).astype(BF16)
                    mix_s[h, :, cols] = mix_s[h, :, cols] * jnp.exp2((old - top) * SCALE) + dot(v0_s[h], p)
            lax.fori_loop(0, HEADS, head, None)
        lax.fori_loop(0, UNITS, unit, None)

    lax.fori_loop(0, TILES, finish, None)

    wo_copy.wait()
    wide = 512

    def heads_of(c):
        return pl.ds(pl.multiple_of(c * WIDE, WIDE), WIDE)

    def out_own(n, _):
        cols = pl.ds(pl.multiple_of(n * wide, wide), wide)
        yacc_s[:, cols] = dot(og_s[:, heads_of(core)], wo_s[heads_of(core), cols])
    lax.fori_loop(0, D // wide, out_own, None)

    for p in range(TILES):
        o_copy(p).wait_recv()

    def y_copy(n):
        cols = pl.ds(pl.multiple_of(n * wide, wide), wide)
        return pltpu.make_async_copy(y_s.at[:, cols], y_ref.at[:, cols], y_sem.at[n])

    def out_other(n, _):
        cols = pl.ds(pl.multiple_of(n * wide, wide), wide)
        y = yacc_s[:, cols] + dot(og_s[:, heads_of(1 - core)], wo_s[heads_of(1 - core), cols])
        y_s[:, cols] = (xs[own_rows, cols].astype(F32) + y).astype(BF16)
        y_copy(n).start()
    lax.fori_loop(0, D // wide, out_other, None)

    for p in range(TILES):
        o_copy(p).wait_send()
    for n in range(D // wide):
        y_copy(n).wait()

    @pl.when(chip == 0)
    def _():
        for j in range(UNITS):
            link(j).wait_send()

    @pl.when(chip == 1)
    def _():
        for j in range(UNITS):
            forward(j).wait_send()


def solution(mesh):
    table = rope_table()

    def step(x, gain, wq, wk, wv, wo):
        hbm = pl.BlockSpec(memory_space=pl.ANY)
        vmem = pltpu.VMEM
        dma = pltpu.SemaphoreType.DMA
        return pl.pallas_call(
            kernel,
            out_shape=jax.ShapeDtypeStruct((OWN, D), BF16),
            in_specs=[hbm, pl.BlockSpec(memory_space=vmem), hbm, hbm, hbm, hbm, hbm],
            out_specs=hbm,
            scratch_shapes=[
                vmem((CHIP, D), BF16), vmem((UNITS, UNIT, D), BF16), vmem((OWN, D), BF16), vmem((3, TILES, D, TILE), BF16),
                vmem((D, D), BF16), vmem((HEADS, CHIP, HEAD), BF16), vmem((HEADS, CHIP, HEAD), BF16), vmem((HEADS, VROWS, CHIP), BF16),
                vmem((HEADS, UNIT, HEAD), BF16), vmem((HEADS, VROWS, UNIT), BF16), vmem((OWN, HEAD), F32), vmem((OWN, HEAD), F32),
                vmem((2 * CHIP, HEAD), F32), vmem((HEADS, 1, CHIP), F32), vmem((HEADS, VROWS, CHIP), F32), vmem((OWN, D), BF16),
                vmem((TILES, OWN, TILE), BF16), vmem((OWN, D), F32), vmem((OWN, D), BF16),
                dma, dma((3, TILES)), dma, dma, dma((2,)), dma((UNITS,)), dma((UNITS,)), dma((UNITS,)), dma((UNITS,)),
                dma((TILES,)), dma((TILES,)), dma((D // 512,)),
            ],
            compiler_params=pltpu.CompilerParams(collective_id=0, has_side_effects=True, vmem_limit_bytes=66 * 10**6),
            cost_estimate=pl.CostEstimate(flops=40 * 10**9, bytes_accessed=36 * 2**20, transcendentals=13 * 10**6),
        )(x, gain.reshape(1, D), wq, wk, wv, wo, jnp.asarray(table))

    tokens, whole = P(("dp", "sp"), None), P(None, None)
    return jax.shard_map(step, mesh=mesh, in_specs=(tokens, P(None), whole, whole, whole, whole), out_specs=tokens, check_vma=False)
```

```python
import functools

import jax
import jax.numpy as jnp
import numpy as np
from jax import lax
from jax.experimental import pallas as pl
from jax.experimental.pallas import tpu as pltpu
from jax.sharding import PartitionSpec as P

HEAD = 128
THETA = 10000
D = 2048
OWN = 512
CHIP = 1024
HEADS = 8
WIDE = HEADS * HEAD
TILE = 256
TILES = WIDE // TILE
PARTS = 4
PART = OWN // PARTS
UNITS = ((0, 2), (2, 3), (3, 4))
MOST = 2 * 2 * PART
HIDDEN = -2e30
LOG2E = 1.4426950408889634
SCALE = HEAD**-0.5 * LOG2E
VROWS = HEAD + 16
MESH = pl.DeviceIdType.MESH
F32, BF16 = jnp.float32, jnp.bfloat16


def rope_table():
    half = HEAD // 2
    place = np.arange(2 * CHIP, dtype=np.float32)[:, None]
    angle = place * np.power(np.float32(THETA), -np.arange(half, dtype=np.float32) / np.float32(half)).astype(np.float32)
    return np.concatenate([np.cos(angle), np.sin(angle)], -1).astype(np.float32)


def dot(a, b, ca=1, cb=0):
    return lax.dot_general(a, b, (((ca,), (cb,)), ((), ())), preferred_element_type=F32)


def kernel(x_ref, gain_ref, wq_ref, wk_ref, wv_ref, wo_ref, rope_ref, y_ref,
           xs, x0, a_s, a0, w_s, wo_s, q_s, k_s, v_s, k0_s, v0_s, cos_s, sin_s, rope_s, top_s, mix_s, og_s, os_s, yacc_s, y_s,
           x_sem, w_sem, wo_sem, rope_sem, pair_send, pair_recv, link_send, link_recv, fwd_send, fwd_recv, o_send, o_recv, y_sem):
    me = lax.axis_index("sp")
    chip, core = lax.div(me, 2), lax.rem(me, 2)
    partner, across = 2 * chip + 1 - core, lax.rem(me + 2, 4)

    barrier = pltpu.get_barrier_semaphore()
    for other in (partner, across):
        pl.semaphore_signal(barrier, inc=1, device_id={"sp": other}, device_id_type=MESH)
    pl.semaphore_wait(barrier, 2)

    def part(j):
        return pl.ds(j * PART, PART)

    def link(j):
        return pltpu.make_async_remote_copy(src_ref=x_ref.at[part(j)], dst_ref=x0.at[part(j)], send_sem=link_send.at[j],
                                            recv_sem=link_recv.at[j], device_id={"sp": across}, device_id_type=MESH)

    def forward(j):
        rows = a0.at[j, pl.ds(core * PART, PART)]
        return pltpu.make_async_remote_copy(src_ref=rows, dst_ref=rows, send_sem=fwd_send.at[j], recv_sem=fwd_recv.at[j],
                                            device_id={"sp": partner}, device_id_type=MESH)

    own_rows = pl.ds(core * OWN, OWN)
    pair = pltpu.make_async_remote_copy(src_ref=a_s.at[own_rows], dst_ref=a_s.at[own_rows], send_sem=pair_send, recv_sem=pair_recv,
                                        device_id={"sp": partner}, device_id_type=MESH)
    rope_copy = pltpu.make_async_copy(rope_ref, rope_s, rope_sem)
    wo_copy = pltpu.make_async_copy(wo_ref, wo_s, wo_sem)

    def x_copy(j):
        return pltpu.make_async_copy(x_ref.at[part(j)], xs.at[part(j)], x_sem.at[j])

    def w_copy(n, which):
        ref = (wq_ref, wk_ref, wv_ref)[which]
        cols = pl.ds(pl.multiple_of(core * WIDE + n * TILE, TILE), TILE)
        return pltpu.make_async_copy(ref.at[:, cols], w_s.at[which, n], w_sem.at[which, n])

    for j in range(PARTS):
        x_copy(j).start()

    @pl.when(chip == 0)
    def _():
        for j in range(PARTS):
            link(j).start()

    for which in range(3):
        w_copy(0, which).start()
    rope_copy.start()
    for n in range(1, TILES):
        for which in range(3):
            w_copy(n, which).start()
    wo_copy.start()

    v_s[:, HEAD:, :] = jnp.ones((HEADS, VROWS - HEAD, CHIP), BF16)
    v0_s[:, HEAD:, :] = jnp.ones((HEADS, VROWS - HEAD, MOST), BF16)

    def norm(get, put, count):
        def step(i, _):
            for at in range(0, 64, 16):
                at = pl.multiple_of(i * 64 + at, 16)
                wide = get(at).astype(F32)
                scale = lax.rsqrt(jnp.mean(wide * wide, -1, keepdims=True) + 1e-6)
                put(at, (wide * scale * gain_ref[...].astype(F32)[None]).astype(BF16))
        lax.fori_loop(0, count // 64, step, None)

    def angles(at, rows, to):
        t = rope_s[pl.ds(at, rows), :]
        r = pltpu.roll(t, 64, 1)
        low = lax.broadcasted_iota(jnp.int32, t.shape, 1) < 64
        cos_s[to : to + rows, :] = jnp.where(low, t, r)
        sin_s[to : to + rows, :] = jnp.where(low, -r, t)

    def turn(t, rows):
        t = t.astype(BF16).astype(F32)
        return (t * cos_s[:rows, :] + pltpu.roll(t, 64, 1) * sin_s[:rows, :]).astype(BF16)

    def put_own(at, rows):
        a_s[pl.ds(core * OWN + at, 16), :] = rows

    for j in range(PARTS):
        x_copy(j).wait()
    norm(lambda at: xs[pl.ds(at, 16), :], put_own, OWN)
    rope_copy.wait()

    def project(half, first):
        rows = pl.ds(pl.multiple_of(half * OWN, OWN), OWN)
        angles(pl.multiple_of(chip * CHIP + half * OWN, OWN), OWN, 0)
        if first:
            pair.start()

        def step(n, _):
            if first:
                for which in range(3):
                    w_copy(n, which).wait()
            a = a_s[rows, :]
            q, k, v = (dot(a, w_s[which, n]) for which in range(3))
            for h in range(2):
                cols = slice(h * HEAD, (h + 1) * HEAD)
                q_s[2 * n + h, :, rows] = turn(q[:, cols], OWN).T
                k_s[2 * n + h, rows, :] = turn(k[:, cols], OWN)
                v_s[2 * n + h, :HEAD, rows] = v[:, cols].astype(BF16).T
        lax.fori_loop(0, TILES, step, None)

    project(core, True)
    pair.wait_recv()
    project(1 - core, False)

    def relay(j):
        link(j).wait_recv()

        def put(at, rows):
            a0[j, pl.ds(core * PART + at, 16), :] = rows
        norm(lambda at: x0[pl.ds(j * PART + at, 16), :], put, PART)
        forward(j).start()

    def within(p, _):
        jobs = [(2 * p + h, b) for h in range(2) for b in range(CHIP // 256)]
        scores = [dot(k_s[h, : (b + 1) * 256, :], q_s[h, :, b * 256 : (b + 1) * 256]) for h, b in jobs]
        ok = lax.broadcasted_iota(jnp.int32, (256, 256), 1) >= lax.broadcasted_iota(jnp.int32, (256, 256), 0)
        weights = []
        for (h, b), s in zip(jobs, scores):
            last = jnp.where(ok, s[b * 256 :], HIDDEN)
            s = jnp.concatenate([s[: b * 256], last], 0) if b else last
            top = s.max(0, keepdims=True)
            top_s[h, :, b * 256 : (b + 1) * 256] = top
            weights.append(jnp.exp2((s - top) * SCALE).astype(BF16))
        for (h, b), p in zip(jobs, weights):
            mix_s[h, :, b * 256 : (b + 1) * 256] = dot(v_s[h, :, : (b + 1) * 256], p)

    def o_copy(p):
        cols = pl.ds(pl.multiple_of((core * TILES + p) * TILE, TILE), TILE)
        return pltpu.make_async_remote_copy(src_ref=os_s.at[p], dst_ref=og_s.at[:, cols], send_sem=o_send.at[p], recv_sem=o_recv.at[p],
                                            device_id={"sp": partner}, device_id_type=MESH)

    def finish(p, _):
        for h in range(2):
            def result(half):
                cols = pl.ds(pl.multiple_of(half * OWN, OWN), OWN)
                return (mix_s[2 * p + h, :HEAD, cols] * (1 / mix_s[2 * p + h, HEAD : HEAD + 1, cols])).T.astype(BF16)
            os_s[p, :, h * HEAD : (h + 1) * HEAD] = result(1 - core)
            og_s[:, pl.ds(pl.multiple_of((core * TILES + p) * TILE + h * HEAD, HEAD), HEAD)] = result(core)
        o_copy(p).start()

    def keys(first, last):
        count = (last - first) * 2 * PART
        for j in range(first, last):
            forward(j).wait_recv()
            for of in range(2):
                angles(of * OWN + j * PART, PART, (j - first) * 2 * PART + of * PART)

        def step(n, _):
            a = a0[first:last].reshape(count, D)
            k, v = (dot(a, w_s[which, n]) for which in (1, 2))
            for h in range(2):
                cols = slice(h * HEAD, (h + 1) * HEAD)
                k0_s[2 * n + h, :count, :] = turn(k[:, cols], count)
                v0_s[2 * n + h, :HEAD, :count] = v[:, cols].astype(BF16).T
        lax.fori_loop(0, TILES, step, None)

    def between(count, done):
        def step(p, _):
            jobs = [(2 * p + h, slice(c, c + 512)) for h in range(2) for c in range(0, CHIP, 512)]
            scores = [dot(k0_s[h, :count], q_s[h, :, cols]) for h, cols in jobs]
            weights = []
            for (h, cols), s in zip(jobs, scores):
                old = top_s[h, :, cols]
                top = jnp.maximum(old, s.max(0, keepdims=True))
                top_s[h, :, cols] = top
                weights.append((jnp.exp2((s - top) * SCALE).astype(BF16), jnp.exp2((old - top) * SCALE)))
            for (h, cols), (w, keep) in zip(jobs, weights):
                mix_s[h, :, cols] = mix_s[h, :, cols] * keep + dot(v0_s[h, :, :count], w)
            if done:
                finish(p, None)
        return step

    half = TILES // 2

    @pl.when(chip == 0)
    def _():
        lax.fori_loop(0, TILES, within, None)
        lax.fori_loop(0, TILES, finish, None)

    @pl.when(chip == 1)
    def _():
        relay(0)
        lax.fori_loop(0, half, within, None)
        relay(1)
        lax.fori_loop(half, TILES, within, None)
        for i, (first, last) in enumerate(UNITS):
            keys(first, last)
            step = between((last - first) * 2 * PART, last == PARTS)
            if last < PARTS:
                lax.fori_loop(0, half, step, None)
                relay(last)
                lax.fori_loop(half, TILES, step, None)
            else:
                lax.fori_loop(0, TILES, step, None)

    wo_copy.wait()
    wide = 512

    def heads_of(c):
        return pl.ds(pl.multiple_of(c * WIDE, WIDE), WIDE)

    def out_own(n, _):
        cols = pl.ds(pl.multiple_of(n * wide, wide), wide)
        yacc_s[:, cols] = dot(og_s[:, heads_of(core)], wo_s[heads_of(core), cols])
    lax.fori_loop(0, D // wide, out_own, None)

    for p in range(TILES):
        o_copy(p).wait_recv()

    def y_copy(n):
        cols = pl.ds(pl.multiple_of(n * wide, wide), wide)
        return pltpu.make_async_copy(y_s.at[:, cols], y_ref.at[:, cols], y_sem.at[n])

    def out_other(n, _):
        cols = pl.ds(pl.multiple_of(n * wide, wide), wide)
        y = yacc_s[:, cols] + dot(og_s[:, heads_of(1 - core)], wo_s[heads_of(1 - core), cols])
        y_s[:, cols] = (xs[:, cols].astype(F32) + y).astype(BF16)
        y_copy(n).start()
    lax.fori_loop(0, D // wide, out_other, None)

    pair.wait_send()
    for p in range(TILES):
        o_copy(p).wait_send()
    for n in range(D // wide):
        y_copy(n).wait()

    @pl.when(chip == 0)
    def _():
        for j in range(PARTS):
            link(j).wait_send()

    @pl.when(chip == 1)
    def _():
        for j in range(PARTS):
            forward(j).wait_send()


def solution(mesh):
    table = rope_table()

    def step(x, gain, wq, wk, wv, wo):
        hbm = pl.BlockSpec(memory_space=pl.ANY)
        vmem = pltpu.VMEM
        dma = pltpu.SemaphoreType.DMA
        return pl.pallas_call(
            kernel,
            out_shape=jax.ShapeDtypeStruct((OWN, D), BF16),
            in_specs=[hbm, pl.BlockSpec(memory_space=vmem), hbm, hbm, hbm, hbm, hbm],
            out_specs=hbm,
            scratch_shapes=[
                vmem((OWN, D), BF16), vmem((OWN, D), BF16), vmem((CHIP, D), BF16), vmem((PARTS, 2 * PART, D), BF16),
                vmem((3, TILES, D, TILE), BF16), vmem((D, D), BF16),
                vmem((HEADS, HEAD, CHIP), BF16), vmem((HEADS, CHIP, HEAD), BF16), vmem((HEADS, VROWS, CHIP), BF16),
                vmem((HEADS, MOST, HEAD), BF16), vmem((HEADS, VROWS, MOST), BF16), vmem((OWN, HEAD), F32), vmem((OWN, HEAD), F32),
                vmem((2 * CHIP, HEAD), F32), vmem((HEADS, 1, CHIP), F32), vmem((HEADS, VROWS, CHIP), F32), vmem((OWN, D), BF16),
                vmem((TILES, OWN, TILE), BF16), vmem((OWN, D), F32), vmem((OWN, D), BF16),
                dma((PARTS,)), dma((3, TILES)), dma, dma, dma, dma, dma((PARTS,)), dma((PARTS,)), dma((PARTS,)), dma((PARTS,)),
                dma((TILES,)), dma((TILES,)), dma((D // 512,)),
            ],
            compiler_params=pltpu.CompilerParams(collective_id=0, has_side_effects=True, vmem_limit_bytes=66 * 10**6),
            cost_estimate=pl.CostEstimate(flops=40 * 10**9, bytes_accessed=36 * 2**20, transcendentals=13 * 10**6),
        )(x, gain, wq, wk, wv, wo, jnp.asarray(table))

    tokens, whole = P(("dp", "sp"), None), P(None, None)
    return jax.shard_map(step, mesh=mesh, in_specs=(tokens, P(None), whole, whole, whole, whole), out_specs=tokens, check_vma=False)
```

```python
import functools

import jax
import jax.numpy as jnp
import numpy as np
from jax import lax
from jax.experimental import pallas as pl
from jax.experimental.pallas import tpu as pltpu
from jax.sharding import PartitionSpec as P

HEAD = 128
THETA = 10000
D = 2048
OWN = 512
CHIP = 1024
HEADS = 8
WIDE = HEADS * HEAD
TILE = 256
TILES = WIDE // TILE
PARTS = 4
PART = OWN // PARTS
UNITS = ((0, 2), (2, 3), (3, 4))
MOST = 2 * 2 * PART
HIDDEN = -2e30
LOG2E = 1.4426950408889634
SCALE = HEAD**-0.5 * LOG2E
VROWS = HEAD + 16
MESH = pl.DeviceIdType.MESH
PER, PER_KEYS = 2, 2
VMEM_LIMIT = 50 * 2**20
F32, BF16 = jnp.float32, jnp.bfloat16


def rope_table():
    half = HEAD // 2
    place = np.arange(2 * CHIP, dtype=np.float32)[:, None]
    angle = place * np.power(np.float32(THETA), -np.arange(half, dtype=np.float32) / np.float32(half)).astype(np.float32)
    return np.concatenate([np.cos(angle), np.sin(angle)], -1).astype(np.float32)


def dot(a, b, ca=1, cb=0):
    return lax.dot_general(a, b, (((ca,), (cb,)), ((), ())), preferred_element_type=F32)


def kernel(x_ref, gain_hbm, wq_ref, wk_ref, wv_ref, rope_ref, og_ref,
           gain_ref, xs, x0, a_s, a0, w_s, q_s, k_s, v_s, k0_s, v0_s, cos_s, sin_s, rope_s, top_s, mix_s, os_s,
           gain_sem, x_sem, w_sem, rope_sem, pair_send, pair_recv, link_send, link_recv, fwd_send, fwd_recv, o_send, o_recv):
    me = lax.axis_index("sp")
    chip, core = lax.div(me, 2), lax.rem(me, 2)
    partner, across = 2 * chip + 1 - core, lax.rem(me + 2, 4)

    barrier = pltpu.get_barrier_semaphore()
    for other in (partner, across):
        pl.semaphore_signal(barrier, inc=1, device_id={"sp": other}, device_id_type=MESH)

    def part(j):
        return pl.ds(j * PART, PART)

    def link(j):
        return pltpu.make_async_remote_copy(src_ref=x_ref.at[part(j)], dst_ref=x0.at[part(j)], send_sem=link_send.at[j],
                                            recv_sem=link_recv.at[j], device_id={"sp": across}, device_id_type=MESH)

    def forward(j):
        rows = a0.at[j, pl.ds(core * PART, PART)]
        return pltpu.make_async_remote_copy(src_ref=rows, dst_ref=rows, send_sem=fwd_send.at[j], recv_sem=fwd_recv.at[j],
                                            device_id={"sp": partner}, device_id_type=MESH)

    own_rows = pl.ds(core * OWN, OWN)
    pair = pltpu.make_async_remote_copy(src_ref=a_s.at[own_rows], dst_ref=a_s.at[own_rows], send_sem=pair_send, recv_sem=pair_recv,
                                        device_id={"sp": partner}, device_id_type=MESH)
    rope_copy = pltpu.make_async_copy(rope_ref, rope_s, rope_sem)

    def x_copy(j):
        return pltpu.make_async_copy(x_ref.at[part(j)], xs.at[part(j)], x_sem.at[j])

    def w_copy(n, which):
        ref = (wq_ref, wk_ref, wv_ref)[which]
        cols = pl.ds(pl.multiple_of(core * WIDE + n * TILE, TILE), TILE)
        return pltpu.make_async_copy(ref.at[:, cols], w_s.at[which, n], w_sem.at[which, n])

    gain_copy = pltpu.make_async_copy(gain_hbm, gain_ref, gain_sem)
    gain_copy.start()
    for j in range(PARTS):
        x_copy(j).start()
    rope_copy.start()
    for which in range(3):
        w_copy(0, which).start()

    pl.semaphore_wait(barrier, 2)

    @pl.when(chip == 0)
    def _():
        for j in range(PARTS):
            link(j).start()

    v_s[:, HEAD:, :] = jnp.ones((HEADS, VROWS - HEAD, CHIP), BF16)
    v0_s[:, HEAD:, :] = jnp.ones((HEADS, VROWS - HEAD, MOST), BF16)

    def norm(get, put, count):
        def step(i, _):
            for at in range(0, 64, 16):
                at = pl.multiple_of(i * 64 + at, 16)
                wide = get(at).astype(F32)
                scale = lax.rsqrt(jnp.mean(wide * wide, -1, keepdims=True) + 1e-6)
                put(at, (wide * scale * gain_ref[...].astype(F32)[None]).astype(BF16))
        lax.fori_loop(0, count // 64, step, None)

    def angles(at, rows, to):
        t = rope_s[pl.ds(at, rows), :]
        r = pltpu.roll(t, 64, 1)
        low = lax.broadcasted_iota(jnp.int32, t.shape, 1) < 64
        cos_s[to : to + rows, :] = jnp.where(low, t, r)
        sin_s[to : to + rows, :] = jnp.where(low, -r, t)

    def turn(t, rows):
        t = t.astype(BF16).astype(F32)
        return (t * cos_s[:rows, :] + pltpu.roll(t, 64, 1) * sin_s[:rows, :]).astype(BF16)

    def put_own(at, rows):
        a_s[pl.ds(core * OWN + at, 16), :] = rows

    gain_copy.wait()
    for j in range(PARTS):
        x_copy(j).wait()
    for n in range(1, TILES):
        for which in range(3):
            w_copy(n, which).start()
    norm(lambda at: xs[pl.ds(at, 16), :], put_own, OWN)
    rope_copy.wait()

    def project(half, first):
        rows = pl.ds(pl.multiple_of(half * OWN, OWN), OWN)
        angles(pl.multiple_of(chip * CHIP + half * OWN, OWN), OWN, 0)
        if first:
            pair.start()

        def step(i, _):
            if first:
                for n in range(PER):
                    for which in range(3):
                        w_copy(PER * i + n, which).wait()
            a = a_s[rows, :]
            for n in range(PER):
                n = PER * i + n
                q, k, v = (dot(a, w_s[which, n]) for which in range(3))
                for h in range(2):
                    cols = slice(h * HEAD, (h + 1) * HEAD)
                    q_s[2 * n + h, :, rows] = turn(q[:, cols], OWN).T
                    k_s[2 * n + h, rows, :] = turn(k[:, cols], OWN)
                    v_s[2 * n + h, :HEAD, rows] = v[:, cols].astype(BF16).T
        lax.fori_loop(0, TILES // PER, step, None)

    project(core, True)
    pair.wait_recv()
    project(1 - core, False)

    def relay(j):
        link(j).wait_recv()

        def put(at, rows):
            a0[j, pl.ds(core * PART + at, 16), :] = rows
        norm(lambda at: x0[pl.ds(j * PART + at, 16), :], put, PART)
        forward(j).start()

    def within(p, _):
        jobs = [(2 * p + h, b) for h in range(2) for b in range(CHIP // 256)]
        scores = [dot(k_s[h, : (b + 1) * 256, :], q_s[h, :, b * 256 : (b + 1) * 256]) for h, b in jobs]
        ok = lax.broadcasted_iota(jnp.int32, (256, 256), 1) >= lax.broadcasted_iota(jnp.int32, (256, 256), 0)
        weights = []
        for (h, b), s in zip(jobs, scores):
            last = jnp.where(ok, s[b * 256 :], HIDDEN)
            s = jnp.concatenate([s[: b * 256], last], 0) if b else last
            top = s.max(0, keepdims=True)
            top_s[h, :, b * 256 : (b + 1) * 256] = top
            weights.append(jnp.exp2((s - top) * SCALE).astype(BF16))
        for (h, b), p in zip(jobs, weights):
            mix_s[h, :, b * 256 : (b + 1) * 256] = dot(v_s[h, :, : (b + 1) * 256], p)

    def o_cols(p):
        return pl.ds(pl.multiple_of((core * TILES + p) * TILE, TILE), TILE)

    def o_copy(p):
        return pltpu.make_async_remote_copy(src_ref=os_s.at[p], dst_ref=og_ref.at[:, o_cols(p)], send_sem=o_send.at[p],
                                            recv_sem=o_recv.at[p], device_id={"sp": partner}, device_id_type=MESH)

    def finish(p, _):
        for h in range(2):
            def result(half):
                cols = pl.ds(pl.multiple_of(half * OWN, OWN), OWN)
                return (mix_s[2 * p + h, :HEAD, cols] * (1 / mix_s[2 * p + h, HEAD : HEAD + 1, cols])).T.astype(BF16)
            os_s[p, :, h * HEAD : (h + 1) * HEAD] = result(1 - core)
            og_ref[:, pl.ds(pl.multiple_of((core * TILES + p) * TILE + h * HEAD, HEAD), HEAD)] = result(core)
        o_copy(p).start()

    def keys(first, last):
        count = (last - first) * 2 * PART
        for j in range(first, last):
            forward(j).wait_recv()
            for of in range(2):
                angles(of * OWN + j * PART, PART, (j - first) * 2 * PART + of * PART)

        per = PER_KEYS * 512 // count

        def step(i, _):
            a = a0[first:last].reshape(count, D)
            for n in range(per):
                n = per * i + n
                k, v = (dot(a, w_s[which, n]) for which in (1, 2))
                for h in range(2):
                    cols = slice(h * HEAD, (h + 1) * HEAD)
                    k0_s[2 * n + h, :count, :] = turn(k[:, cols], count)
                    v0_s[2 * n + h, :HEAD, :count] = v[:, cols].astype(BF16).T
        lax.fori_loop(0, TILES // per, step, None)

    def between(count, done):
        def step(p, _):
            jobs = [(2 * p + h, slice(c, c + 512)) for h in range(2) for c in range(0, CHIP, 512)]
            scores = [dot(k0_s[h, :count], q_s[h, :, cols]) for h, cols in jobs]
            weights = []
            for (h, cols), s in zip(jobs, scores):
                old = top_s[h, :, cols]
                top = jnp.maximum(old, s.max(0, keepdims=True))
                top_s[h, :, cols] = top
                weights.append((jnp.exp2((s - top) * SCALE).astype(BF16), jnp.exp2((old - top) * SCALE)))
            for (h, cols), (w, keep) in zip(jobs, weights):
                mix_s[h, :, cols] = mix_s[h, :, cols] * keep + dot(v0_s[h, :, :count], w)
            if done:
                finish(p, None)
        return step

    half = TILES // 2

    @pl.when(chip == 0)
    def _():
        lax.fori_loop(0, TILES, within, None)
        lax.fori_loop(0, TILES, finish, None)

    @pl.when(chip == 1)
    def _():
        relay(0)
        lax.fori_loop(0, half, within, None)
        relay(1)
        lax.fori_loop(half, TILES, within, None)
        for i, (first, last) in enumerate(UNITS):
            keys(first, last)
            step = between((last - first) * 2 * PART, last == PARTS)
            if last < PARTS:
                early = TILES - 1 if last == PARTS - 1 else half
                lax.fori_loop(0, early, step, None)
                relay(last)
                lax.fori_loop(early, TILES, step, None)
            else:
                lax.fori_loop(0, TILES, step, None)

    pair.wait_send()
    for p in range(TILES):
        o_copy(p).wait()

    @pl.when(chip == 0)
    def _():
        for j in range(PARTS):
            link(j).wait_send()

    @pl.when(chip == 1)
    def _():
        for j in range(PARTS):
            forward(j).wait_send()


def out_kernel(o_ref, wo_ref, x_ref, y_ref, y_s, y_sem):
    wide = 512

    def y_copy(n):
        cols = pl.ds(pl.multiple_of(n * wide, wide), wide)
        return pltpu.make_async_copy(y_s.at[:, cols], y_ref.at[:, cols], y_sem.at[n])

    def step(n, _):
        cols = pl.ds(pl.multiple_of(n * wide, wide), wide)
        y_s[:, cols] = (x_ref[:, cols].astype(F32) + dot(o_ref[...], wo_ref[:, cols])).astype(BF16)
        y_copy(n).start()
    lax.fori_loop(0, D // wide, step, None)
    for n in range(D // wide):
        y_copy(n).wait()


def project_out(o, wo, x):
    whole = pl.BlockSpec(memory_space=pltpu.VMEM)
    return pl.pallas_call(
        out_kernel,
        out_shape=jax.ShapeDtypeStruct((OWN, D), BF16),
        in_specs=[whole] * 3,
        out_specs=pl.BlockSpec(memory_space=pltpu.HBM),
        scratch_shapes=[pltpu.VMEM((OWN, D), BF16), pltpu.SemaphoreType.DMA((D // 512,))],
        compiler_params=pltpu.CompilerParams(vmem_limit_bytes=32 * 2**20),
        cost_estimate=pl.CostEstimate(flops=2 * OWN * D * D, bytes_accessed=14 * 2**20, transcendentals=0),
    )(o, wo, x)


def in_hbm(t):
    return pltpu.with_memory_space_constraint(t, pltpu.HBM)


def solution(mesh):
    table = rope_table()

    def step(x, gain, wq, wk, wv, wo):
        hbm = pl.BlockSpec(memory_space=pl.ANY)
        vmem = pltpu.VMEM
        dma = pltpu.SemaphoreType.DMA
        o = pl.pallas_call(
            kernel,
            out_shape=jax.ShapeDtypeStruct((OWN, D), BF16),
            in_specs=[hbm] * 6,
            out_specs=pl.BlockSpec(memory_space=vmem),
            scratch_shapes=[
                vmem((D,), BF16), vmem((OWN, D), BF16), vmem((OWN, D), BF16), vmem((CHIP, D), BF16), vmem((PARTS, 2 * PART, D), BF16),
                vmem((3, TILES, D, TILE), BF16),
                vmem((HEADS, HEAD, CHIP), BF16), vmem((HEADS, CHIP, HEAD), BF16), vmem((HEADS, VROWS, CHIP), BF16),
                vmem((HEADS, MOST, HEAD), BF16), vmem((HEADS, VROWS, MOST), BF16), vmem((OWN, HEAD), F32), vmem((OWN, HEAD), F32),
                vmem((2 * CHIP, HEAD), F32), vmem((HEADS, 1, CHIP), F32), vmem((HEADS, VROWS, CHIP), F32),
                vmem((TILES, OWN, TILE), BF16),
                dma, dma((PARTS,)), dma((3, TILES)), dma, dma, dma, dma((PARTS,)), dma((PARTS,)), dma((PARTS,)), dma((PARTS,)),
                dma((TILES,)), dma((TILES,)),
            ],
            compiler_params=pltpu.CompilerParams(collective_id=0, has_side_effects=True, vmem_limit_bytes=VMEM_LIMIT),
            cost_estimate=pl.CostEstimate(flops=40 * 10**9, bytes_accessed=36 * 2**20, transcendentals=13 * 10**6),
        )(x, in_hbm(gain), wq, wk, wv, in_hbm(jnp.asarray(table)))
        return project_out(o, wo, x)

    tokens, whole = P(("dp", "sp"), None), P(None, None)
    return jax.shard_map(step, mesh=mesh, in_specs=(tokens, P(None), whole, whole, whole, whole), out_specs=tokens, check_vma=False)
```

```python
import functools

import jax
import jax.numpy as jnp
import numpy as np
from jax import lax
from jax.experimental import pallas as pl
from jax.experimental.pallas import tpu as pltpu
from jax.sharding import PartitionSpec as P

HEAD = 128
THETA = 10000
D = 2048
OWN = 512
CHIP = 1024
HEADS = 8
WIDE = HEADS * HEAD
TILE = 256
TILES = WIDE // TILE
PARTS = 4
PART = OWN // PARTS
LAST = PARTS - 1
COLS = D // 2
MOST = 2 * 2 * PART
HIDDEN = -2e30
LOG2E = 1.4426950408889634
SCALE = HEAD**-0.5 * LOG2E
VROWS = HEAD + 16
MESH = pl.DeviceIdType.MESH
PER, PER_KEYS, PER_LAST = 2, 2, 4
VMEM_LIMIT = 50 * 2**20
F32, BF16 = jnp.float32, jnp.bfloat16


def rope_table():
    half = HEAD // 2
    place = np.arange(2 * CHIP, dtype=np.float32)[:, None]
    angle = place * np.power(np.float32(THETA), -np.arange(half, dtype=np.float32) / np.float32(half)).astype(np.float32)
    return np.concatenate([np.cos(angle), np.sin(angle)], -1).astype(np.float32)


def dot(a, b, ca=1, cb=0):
    return lax.dot_general(a, b, (((ca,), (cb,)), ((), ())), preferred_element_type=F32)


def kernel(x_ref, gain_hbm, wq_ref, wk_ref, wv_ref, rope_ref, og_ref,
           gain_ref, xs, x0, a_s, a0, w_s, q_s, k_s, v_s, k0_s, v0_s, cos_s, sin_s, rope_s, top_s, mix_s, os_s, kv_s,
           gain_sem, x_sem, w_sem, rope_sem, pair_send, pair_recv, link_send, link_recv, fwd_send, fwd_recv, o_send, o_recv):
    me = lax.axis_index("sp")
    chip, core = lax.div(me, 2), lax.rem(me, 2)
    partner, across = 2 * chip + 1 - core, lax.rem(me + 2, 4)

    barrier = pltpu.get_barrier_semaphore()
    for other in (partner, across):
        pl.semaphore_signal(barrier, inc=1, device_id={"sp": other}, device_id_type=MESH)

    def part(j):
        return pl.ds(j * PART, PART)

    def link(j):
        return pltpu.make_async_remote_copy(src_ref=x_ref.at[part(j)], dst_ref=x0.at[part(j)], send_sem=link_send.at[j],
                                            recv_sem=link_recv.at[j], device_id={"sp": across}, device_id_type=MESH)

    def forward(j):
        rows = a0.at[j, pl.ds(core * PART, PART)]
        return pltpu.make_async_remote_copy(src_ref=rows, dst_ref=rows, send_sem=fwd_send.at[j], recv_sem=fwd_recv.at[j],
                                            device_id={"sp": partner}, device_id_type=MESH)

    def halves(c):
        return a0.at[LAST, pl.ds(core * PART, PART), pl.ds(c * COLS, COLS)]

    def link_half(c):
        return pltpu.make_async_remote_copy(
            src_ref=a_s.at[pl.ds(core * OWN + LAST * PART, PART), pl.ds(c * COLS, COLS)], dst_ref=halves(c), send_sem=link_send.at[LAST + c],
            recv_sem=link_recv.at[LAST + c], device_id={"sp": across}, device_id_type=MESH)

    def forward_half(c):
        return pltpu.make_async_remote_copy(src_ref=halves(c), dst_ref=halves(c), send_sem=fwd_send.at[LAST + c],
                                            recv_sem=fwd_recv.at[LAST + c], device_id={"sp": partner}, device_id_type=MESH)

    own_rows = pl.ds(core * OWN, OWN)
    pair = pltpu.make_async_remote_copy(src_ref=a_s.at[own_rows], dst_ref=a_s.at[own_rows], send_sem=pair_send, recv_sem=pair_recv,
                                        device_id={"sp": partner}, device_id_type=MESH)
    rope_copy = pltpu.make_async_copy(rope_ref, rope_s, rope_sem)

    def x_copy(j):
        return pltpu.make_async_copy(x_ref.at[part(j)], xs.at[part(j)], x_sem.at[j])

    def w_copy(n, which):
        ref = (wq_ref, wk_ref, wv_ref)[which]
        cols = pl.ds(pl.multiple_of(core * WIDE + n * TILE, TILE), TILE)
        return pltpu.make_async_copy(ref.at[:, cols], w_s.at[which, n], w_sem.at[which, n])

    gain_copy = pltpu.make_async_copy(gain_hbm, gain_ref, gain_sem)
    gain_copy.start()
    for j in range(PARTS):
        x_copy(j).start()
    rope_copy.start()
    for which in range(3):
        w_copy(0, which).start()

    pl.semaphore_wait(barrier, 2)

    @pl.when(chip == 0)
    def _():
        for j in range(LAST):
            link(j).start()

    for n in range(1, TILES):
        for which in range(3):
            w_copy(n, which).start()

    v_s[:, HEAD:, :] = jnp.ones((HEADS, VROWS - HEAD, CHIP), BF16)
    v0_s[:, HEAD:, :] = jnp.ones((HEADS, VROWS - HEAD, MOST), BF16)

    def norm(get, put, count):
        def step(i, _):
            for at in range(0, 64, 16):
                at = pl.multiple_of(i * 64 + at, 16)
                wide = get(at).astype(F32)
                scale = lax.rsqrt(jnp.mean(wide * wide, -1, keepdims=True) + 1e-6)
                put(at, (wide * scale * gain_ref[...].astype(F32)[None]).astype(BF16))
        lax.fori_loop(0, count // 64, step, None)

    def angles(at, rows, to):
        t = rope_s[pl.ds(at, rows), :]
        r = pltpu.roll(t, 64, 1)
        low = lax.broadcasted_iota(jnp.int32, t.shape, 1) < 64
        cos_s[to : to + rows, :] = jnp.where(low, t, r)
        sin_s[to : to + rows, :] = jnp.where(low, -r, t)

    def turn(t, rows):
        t = t.astype(BF16).astype(F32)
        return (t * cos_s[:rows, :] + pltpu.roll(t, 64, 1) * sin_s[:rows, :]).astype(BF16)

    def put_own(at, rows):
        a_s[pl.ds(core * OWN + at, 16), :] = rows

    gain_copy.wait()
    for j in range(PARTS):
        x_copy(j).wait()
    norm(lambda at: xs[pl.ds(at, 16), :], put_own, OWN)
    rope_copy.wait()

    @pl.when(chip == 0)
    def _():
        for c in range(2):
            link_half(c).start()
    pair.start()

    def project(i, _):
        of = lax.rem(core + lax.div(i, TILES // PER), 2)
        first = lax.rem(i, TILES // PER) * PER
        rows = pl.ds(pl.multiple_of(of * OWN, OWN), OWN)

        @pl.when(i < TILES // PER)
        def _():
            for n in range(PER):
                for which in range(3):
                    w_copy(first + n, which).wait()

        @pl.when(i == TILES // PER)
        def _():
            pair.wait_recv()

        @pl.when(first == 0)
        def _():
            angles(pl.multiple_of(chip * CHIP + of * OWN, OWN), OWN, 0)
        a = a_s[rows, :]
        for n in range(PER):
            n = first + n
            q, k, v = (dot(a, w_s[which, n]) for which in range(3))
            for h in range(2):
                cols = slice(h * HEAD, (h + 1) * HEAD)
                q_s[2 * n + h, :, rows] = turn(q[:, cols], OWN).T
                k_s[2 * n + h, rows, :] = turn(k[:, cols], OWN)
                v_s[2 * n + h, :HEAD, rows] = v[:, cols].astype(BF16).T
    lax.fori_loop(0, 2 * TILES // PER, project, None)

    def relay(j):
        link(j).wait_recv()

        def put(at, rows):
            a0[j, pl.ds(core * PART + at, 16), :] = rows
        norm(lambda at: x0[pl.ds(j * PART + at, 16), :], put, PART)
        forward(j).start()

    def relay_half(c):
        link_half(c).wait_recv()
        forward_half(c).start()

    def within(p, _):
        jobs = [(2 * p + h, b) for h in range(2) for b in range(CHIP // 256)]
        scores = [dot(k_s[h, : (b + 1) * 256, :], q_s[h, :, b * 256 : (b + 1) * 256]) for h, b in jobs]
        ok = lax.broadcasted_iota(jnp.int32, (256, 256), 1) >= lax.broadcasted_iota(jnp.int32, (256, 256), 0)
        weights = []
        for (h, b), s in zip(jobs, scores):
            last = jnp.where(ok, s[b * 256 :], HIDDEN)
            s = jnp.concatenate([s[: b * 256], last], 0) if b else last
            top = s.max(0, keepdims=True)
            top_s[h, :, b * 256 : (b + 1) * 256] = top
            weights.append(jnp.exp2((s - top) * SCALE).astype(BF16))
        for (h, b), p in zip(jobs, weights):
            mix_s[h, :, b * 256 : (b + 1) * 256] = dot(v_s[h, :, : (b + 1) * 256], p)

    def o_cols(p):
        return pl.ds(pl.multiple_of((core * TILES + p) * TILE, TILE), TILE)

    def o_copy(p):
        return pltpu.make_async_remote_copy(src_ref=os_s.at[p], dst_ref=og_ref.at[:, o_cols(p)], send_sem=o_send.at[p],
                                            recv_sem=o_recv.at[p], device_id={"sp": partner}, device_id_type=MESH)

    def finish(i, own):
        rows = pl.ds(pl.multiple_of(core * OWN if own else (1 - core) * OWN, OWN), OWN)
        for h in range(4):
            o = (mix_s[4 * i + h, :HEAD, rows] * (1 / mix_s[4 * i + h, HEAD : HEAD + 1, rows])).T.astype(BF16)
            if own:
                og_ref[:, pl.ds(pl.multiple_of((core * TILES + 2 * i) * TILE + h * HEAD, HEAD), HEAD)] = o
            else:
                os_s[2 * i + h // 2, :, h % 2 * HEAD : (h % 2 + 1) * HEAD] = o
                if h % 2:
                    o_copy(2 * i + h // 2).start()

    def angles_of(j, to):
        for of in range(2):
            angles(of * OWN + j * PART, PART, to + of * PART)

    def put_keys(n, k, v, count):
        for h in range(2):
            cols = slice(h * HEAD, (h + 1) * HEAD)
            k0_s[2 * n + h, :count, :] = turn(k[:, cols], count)
            v0_s[2 * n + h, :HEAD, :count] = v[:, cols].astype(BF16).T

    def keys(first, last):
        count = (last - first) * 2 * PART
        for j in range(first, last):
            forward(j).wait_recv()
            angles_of(j, (j - first) * 2 * PART)
        per = PER_KEYS * 512 // count

        def step(i, _):
            a = a0[first:last].reshape(count, D)
            for n in range(per):
                n = per * i + n
                k, v = (dot(a, w_s[which, n]) for which in (1, 2))
                put_keys(n, k, v, count)
        lax.fori_loop(0, TILES // per, step, None)

    def last_keys(c):
        forward_half(c).wait_recv()
        if c == 1:
            angles_of(LAST, 0)

        def step(i, _):
            a = a0[LAST, :, c * COLS : (c + 1) * COLS]
            for n in range(PER_LAST):
                n = PER_LAST * i + n
                k, v = (dot(a, w_s[which, n, c * COLS : (c + 1) * COLS, :]) for which in (1, 2))
                if c == 0:
                    kv_s[0, n], kv_s[1, n] = k, v
                else:
                    put_keys(n, kv_s[0, n] + k, kv_s[1, n] + v, 2 * PART)
        lax.fori_loop(0, TILES // PER_LAST, step, None)

    def attend(jobs, count):
        scores = [dot(k0_s[h, :count], q_s[h, :, cols]) for h, cols in jobs]
        weights = []
        for (h, cols), s in zip(jobs, scores):
            old = top_s[h, :, cols]
            top = jnp.maximum(old, s.max(0, keepdims=True))
            top_s[h, :, cols] = top
            weights.append((jnp.exp2((s - top) * SCALE).astype(BF16), jnp.exp2((old - top) * SCALE)))
        for (h, cols), (w, keep) in zip(jobs, weights):
            mix_s[h, :, cols] = mix_s[h, :, cols] * keep + dot(v0_s[h, :, :count], w)

    def between(count):
        def step(p, _):
            attend([(2 * p + h, slice(c, c + 512)) for h in range(2) for c in range(0, CHIP, 512)], count)
        return step

    def final(own):
        def step(i, _):
            rows = pl.ds(pl.multiple_of(core * OWN if own else (1 - core) * OWN, OWN), OWN)
            attend([(4 * i + h, rows) for h in range(4)], 2 * PART)
            finish(i, own)
        return step

    half = TILES // 2

    @pl.when(chip == 0)
    def _():
        lax.fori_loop(0, TILES, within, None)
        for own in (False, True):
            lax.fori_loop(0, HEADS // 4, lambda i, _: finish(i, own), None)

    @pl.when(chip == 1)
    def _():
        relay(0)
        lax.fori_loop(0, TILES - 1, within, None)
        relay(1)
        lax.fori_loop(TILES - 1, TILES, within, None)
        keys(0, 2)
        step = between(4 * PART)
        lax.fori_loop(0, half, step, None)
        relay(2)
        lax.fori_loop(half, TILES, step, None)
        keys(2, 3)
        step = between(2 * PART)
        lax.fori_loop(0, half, step, None)
        relay_half(0)
        lax.fori_loop(half, TILES, step, None)
        relay_half(1)
        last_keys(0)
        last_keys(1)
        lax.fori_loop(0, HEADS // 4, final(False), None)
        lax.fori_loop(0, HEADS // 4, final(True), None)

    pair.wait_send()
    for p in range(TILES):
        o_copy(p).wait()

    @pl.when(chip == 0)
    def _():
        for j in range(LAST):
            link(j).wait_send()
        for c in range(2):
            link_half(c).wait_send()

    @pl.when(chip == 1)
    def _():
        for j in range(LAST):
            forward(j).wait_send()
        for c in range(2):
            forward_half(c).wait_send()


def out_kernel(o_ref, wo_ref, x_hbm, y_ref, x_ref, y_s, x_sem, y_sem):
    wide = 512
    x_copy = pltpu.make_async_copy(x_hbm, x_ref, x_sem)
    x_copy.start()

    def y_copy(n):
        cols = pl.ds(pl.multiple_of(n * wide, wide), wide)
        return pltpu.make_async_copy(y_s.at[:, cols], y_ref.at[:, cols], y_sem.at[n])

    def put(n, y):
        cols = pl.ds(pl.multiple_of(n * wide, wide), wide)
        y_s[:, cols] = (x_ref[:, cols].astype(F32) + y).astype(BF16)
        y_copy(n).start()

    first = dot(o_ref[...], wo_ref[:, :wide])
    x_copy.wait()
    put(0, first)

    def step(n, _):
        put(n, dot(o_ref[...], wo_ref[:, pl.ds(pl.multiple_of(n * wide, wide), wide)]))
    lax.fori_loop(1, D // wide, step, None)
    for n in range(D // wide):
        y_copy(n).wait()


def project_out(o, wo, x):
    whole = pl.BlockSpec(memory_space=pltpu.VMEM)
    return pl.pallas_call(
        out_kernel,
        out_shape=jax.ShapeDtypeStruct((OWN, D), BF16),
        in_specs=[whole, whole, pl.BlockSpec(memory_space=pl.ANY)],
        out_specs=pl.BlockSpec(memory_space=pltpu.HBM),
        scratch_shapes=[pltpu.VMEM((OWN, D), BF16)] * 2 + [pltpu.SemaphoreType.DMA, pltpu.SemaphoreType.DMA((D // 512,))],
        compiler_params=pltpu.CompilerParams(vmem_limit_bytes=32 * 2**20),
        cost_estimate=pl.CostEstimate(flops=2 * OWN * D * D, bytes_accessed=14 * 2**20, transcendentals=0),
    )(o, wo, x)


def in_hbm(t):
    return pltpu.with_memory_space_constraint(t, pltpu.HBM)


def solution(mesh):
    table = rope_table()

    def step(x, gain, wq, wk, wv, wo):
        hbm = pl.BlockSpec(memory_space=pl.ANY)
        vmem = pltpu.VMEM
        dma = pltpu.SemaphoreType.DMA
        o = pl.pallas_call(
            kernel,
            out_shape=jax.ShapeDtypeStruct((OWN, D), BF16),
            in_specs=[hbm] * 6,
            out_specs=pl.BlockSpec(memory_space=vmem),
            scratch_shapes=[
                vmem((D,), BF16), vmem((OWN, D), BF16), vmem((OWN, D), BF16), vmem((CHIP, D), BF16), vmem((PARTS, 2 * PART, D), BF16),
                vmem((3, TILES, D, TILE), BF16),
                vmem((HEADS, HEAD, CHIP), BF16), vmem((HEADS, CHIP, HEAD), BF16), vmem((HEADS, VROWS, CHIP), BF16),
                vmem((HEADS, MOST, HEAD), BF16), vmem((HEADS, VROWS, MOST), BF16), vmem((OWN, HEAD), F32), vmem((OWN, HEAD), F32),
                vmem((2 * CHIP, HEAD), F32), vmem((HEADS, 1, CHIP), F32), vmem((HEADS, VROWS, CHIP), F32),
                vmem((TILES, OWN, TILE), BF16), vmem((2, TILES, 2 * PART, TILE), F32),
                dma, dma((PARTS,)), dma((3, TILES)), dma, dma, dma, dma((PARTS + 1,)), dma((PARTS + 1,)), dma((PARTS + 1,)), dma((PARTS + 1,)),
                dma((TILES,)), dma((TILES,)),
            ],
            compiler_params=pltpu.CompilerParams(collective_id=0, has_side_effects=True, vmem_limit_bytes=VMEM_LIMIT),
            cost_estimate=pl.CostEstimate(flops=40 * 10**9, bytes_accessed=36 * 2**20, transcendentals=13 * 10**6),
        )(x, in_hbm(gain), wq, wk, wv, in_hbm(jnp.asarray(table)))
        return project_out(o, wo, in_hbm(x))

    tokens, whole = P(("dp", "sp"), None), P(None, None)
    return jax.shard_map(step, mesh=mesh, in_specs=(tokens, P(None), whole, whole, whole, whole), out_specs=tokens, check_vma=False)
```

```python
import functools

import jax
import jax.numpy as jnp
import numpy as np
from jax import lax
from jax.experimental import pallas as pl
from jax.experimental.pallas import tpu as pltpu
from jax.sharding import PartitionSpec as P

HEAD = 128
THETA = 10000
D = 2048
OWN = 512
CHIP = 1024
HEADS = 8
WIDE = HEADS * HEAD
TILE = 256
TILES = WIDE // TILE
PARTS = 4
PART = OWN // PARTS
LAST = PARTS - 1
COLS = ((0, 1536), (1536, 2048))
MOST = 2 * 2 * PART
HIDDEN = -2e30
LOG2E = 1.4426950408889634
SCALE = HEAD**-0.5 * LOG2E
VROWS = HEAD + 16
MESH = pl.DeviceIdType.MESH
PER, PER_KEYS, PER_LAST = 2, 2, 4
VMEM_LIMIT = 50 * 2**20
F32, BF16 = jnp.float32, jnp.bfloat16


def rope_table():
    half = HEAD // 2
    place = np.arange(2 * CHIP, dtype=np.float32)[:, None]
    angle = place * np.power(np.float32(THETA), -np.arange(half, dtype=np.float32) / np.float32(half)).astype(np.float32)
    return np.concatenate([np.cos(angle), np.sin(angle)], -1).astype(np.float32)


def dot(a, b, ca=1, cb=0):
    return lax.dot_general(a, b, (((ca,), (cb,)), ((), ())), preferred_element_type=F32)


def kernel(x_ref, gain_hbm, wq_ref, wk_ref, wv_ref, rope_ref, og_ref,
           gain_ref, xs, x0, a_s, a0, w_s, q_s, k_s, v_s, k0_s, v0_s, cos_s, sin_s, rope_s, top_s, mix_s, os_s, kv_s,
           gain_sem, x_sem, w_sem, rope_sem, pair_send, pair_recv, link_send, link_recv, fwd_send, fwd_recv, o_send, o_recv):
    me = lax.axis_index("sp")
    chip, core = lax.div(me, 2), lax.rem(me, 2)
    partner, across = 2 * chip + 1 - core, lax.rem(me + 2, 4)

    barrier = pltpu.get_barrier_semaphore()
    for other in (partner, across):
        pl.semaphore_signal(barrier, inc=1, device_id={"sp": other}, device_id_type=MESH)

    def part(j):
        return pl.ds(j * PART, PART)

    def link(j):
        return pltpu.make_async_remote_copy(src_ref=x_ref.at[part(j)], dst_ref=x0.at[part(j)], send_sem=link_send.at[j],
                                            recv_sem=link_recv.at[j], device_id={"sp": across}, device_id_type=MESH)

    def forward(j):
        rows = a0.at[j, pl.ds(core * PART, PART)]
        return pltpu.make_async_remote_copy(src_ref=rows, dst_ref=rows, send_sem=fwd_send.at[j], recv_sem=fwd_recv.at[j],
                                            device_id={"sp": partner}, device_id_type=MESH)

    def columns(c):
        return pl.ds(COLS[c][0], COLS[c][1] - COLS[c][0])

    def piece(c):
        return a0.at[LAST, pl.ds(core * PART, PART), columns(c)]

    def link_piece(c):
        return pltpu.make_async_remote_copy(
            src_ref=a_s.at[pl.ds(core * OWN + LAST * PART, PART), columns(c)], dst_ref=piece(c), send_sem=link_send.at[LAST + c],
            recv_sem=link_recv.at[LAST + c], device_id={"sp": across}, device_id_type=MESH)

    def forward_piece(c):
        return pltpu.make_async_remote_copy(src_ref=piece(c), dst_ref=piece(c), send_sem=fwd_send.at[LAST + c],
                                            recv_sem=fwd_recv.at[LAST + c], device_id={"sp": partner}, device_id_type=MESH)

    own_rows = pl.ds(core * OWN, OWN)
    pair = pltpu.make_async_remote_copy(src_ref=a_s.at[own_rows], dst_ref=a_s.at[own_rows], send_sem=pair_send, recv_sem=pair_recv,
                                        device_id={"sp": partner}, device_id_type=MESH)
    rope_copy = pltpu.make_async_copy(rope_ref, rope_s, rope_sem)

    def x_copy(j):
        return pltpu.make_async_copy(x_ref.at[part(j)], xs.at[part(j)], x_sem.at[j])

    def w_copy(n, which):
        ref = (wq_ref, wk_ref, wv_ref)[which]
        cols = pl.ds(pl.multiple_of(core * WIDE + n * TILE, TILE), TILE)
        return pltpu.make_async_copy(ref.at[:, cols], w_s.at[which, n], w_sem.at[which, n])

    gain_copy = pltpu.make_async_copy(gain_hbm, gain_ref, gain_sem)
    gain_copy.start()
    for j in range(PARTS):
        x_copy(j).start()
    rope_copy.start()
    for which in range(3):
        w_copy(0, which).start()

    pl.semaphore_wait(barrier, 2)

    @pl.when(chip == 0)
    def _():
        for j in range(LAST):
            link(j).start()

    for n in range(1, TILES):
        for which in range(3):
            w_copy(n, which).start()

    v_s[:, HEAD:, :] = jnp.ones((HEADS, VROWS - HEAD, CHIP), BF16)
    v0_s[:, HEAD:, :] = jnp.ones((HEADS, VROWS - HEAD, MOST), BF16)

    def norm(get, put, count):
        def step(i, _):
            for at in range(0, 64, 16):
                at = pl.multiple_of(i * 64 + at, 16)
                wide = get(at).astype(F32)
                scale = lax.rsqrt(jnp.mean(wide * wide, -1, keepdims=True) + 1e-6)
                put(at, (wide * scale * gain_ref[...].astype(F32)[None]).astype(BF16))
        lax.fori_loop(0, count // 64, step, None)

    def angles(at, rows, to):
        t = rope_s[pl.ds(at, rows), :]
        r = pltpu.roll(t, 64, 1)
        low = lax.broadcasted_iota(jnp.int32, t.shape, 1) < 64
        cos_s[to : to + rows, :] = jnp.where(low, t, r)
        sin_s[to : to + rows, :] = jnp.where(low, -r, t)

    def turn(t, rows):
        t = t.astype(BF16).astype(F32)
        return (t * cos_s[:rows, :] + pltpu.roll(t, 64, 1) * sin_s[:rows, :]).astype(BF16)

    def put_own(at, rows):
        a_s[pl.ds(core * OWN + at, 16), :] = rows

    gain_copy.wait()
    for j in range(PARTS):
        x_copy(j).wait()
    norm(lambda at: xs[pl.ds(at, 16), :], put_own, OWN)
    rope_copy.wait()

    @pl.when(chip == 0)
    def _():
        for c in range(2):
            link_piece(c).start()
    pair.start()

    def project(i, _):
        of = lax.rem(core + lax.div(i, TILES // PER), 2)
        first = lax.rem(i, TILES // PER) * PER
        rows = pl.ds(pl.multiple_of(of * OWN, OWN), OWN)

        @pl.when(i < TILES // PER)
        def _():
            for n in range(PER):
                for which in range(3):
                    w_copy(first + n, which).wait()

        @pl.when(i == TILES // PER)
        def _():
            pair.wait_recv()

        @pl.when(first == 0)
        def _():
            angles(pl.multiple_of(chip * CHIP + of * OWN, OWN), OWN, 0)
        a = a_s[rows, :]
        for n in range(PER):
            n = first + n
            q, k, v = (dot(a, w_s[which, n]) for which in range(3))
            for h in range(2):
                cols = slice(h * HEAD, (h + 1) * HEAD)
                q_s[2 * n + h, :, rows] = turn(q[:, cols], OWN).T
                k_s[2 * n + h, rows, :] = turn(k[:, cols], OWN)
                v_s[2 * n + h, :HEAD, rows] = v[:, cols].astype(BF16).T
    lax.fori_loop(0, 2 * TILES // PER, project, None)

    def relay(j):
        link(j).wait_recv()

        def put(at, rows):
            a0[j, pl.ds(core * PART + at, 16), :] = rows
        norm(lambda at: x0[pl.ds(j * PART + at, 16), :], put, PART)
        forward(j).start()

    def relay_piece(c):
        link_piece(c).wait_recv()
        forward_piece(c).start()

    def within(p, _):
        jobs = [(2 * p + h, b) for h in range(2) for b in range(CHIP // 256)]
        scores = [dot(k_s[h, : (b + 1) * 256, :], q_s[h, :, b * 256 : (b + 1) * 256]) for h, b in jobs]
        ok = lax.broadcasted_iota(jnp.int32, (256, 256), 1) >= lax.broadcasted_iota(jnp.int32, (256, 256), 0)
        weights = []
        for (h, b), s in zip(jobs, scores):
            last = jnp.where(ok, s[b * 256 :], HIDDEN)
            s = jnp.concatenate([s[: b * 256], last], 0) if b else last
            top = s.max(0, keepdims=True)
            top_s[h, :, b * 256 : (b + 1) * 256] = top
            weights.append(jnp.exp2((s - top) * SCALE).astype(BF16))
        for (h, b), p in zip(jobs, weights):
            mix_s[h, :, b * 256 : (b + 1) * 256] = dot(v_s[h, :, : (b + 1) * 256], p)

    def o_cols(p):
        return pl.ds(pl.multiple_of((core * TILES + p) * TILE, TILE), TILE)

    def o_copy(p):
        return pltpu.make_async_remote_copy(src_ref=os_s.at[p], dst_ref=og_ref.at[:, o_cols(p)], send_sem=o_send.at[p],
                                            recv_sem=o_recv.at[p], device_id={"sp": partner}, device_id_type=MESH)

    def finish(own):
        rows = pl.ds(pl.multiple_of(core * OWN if own else (1 - core) * OWN, OWN), OWN)
        for h in range(HEADS):
            o = (mix_s[h, :HEAD, rows] * (1 / mix_s[h, HEAD : HEAD + 1, rows])).T.astype(BF16)
            if own:
                og_ref[:, pl.ds(pl.multiple_of(core * WIDE + h * HEAD, HEAD), HEAD)] = o
            else:
                os_s[h // 2, :, h % 2 * HEAD : (h % 2 + 1) * HEAD] = o
                if h % 2:
                    o_copy(h // 2).start()

    def angles_of(j, to):
        for of in range(2):
            angles(of * OWN + j * PART, PART, to + of * PART)

    def put_keys(n, k, v, count):
        for h in range(2):
            cols = slice(h * HEAD, (h + 1) * HEAD)
            k0_s[2 * n + h, :count, :] = turn(k[:, cols], count)
            v0_s[2 * n + h, :HEAD, :count] = v[:, cols].astype(BF16).T

    def keys(first, last):
        count = (last - first) * 2 * PART
        for j in range(first, last):
            forward(j).wait_recv()
            angles_of(j, (j - first) * 2 * PART)
        per = PER_KEYS * 512 // count

        def step(i, _):
            a = a0[first:last].reshape(count, D)
            for n in range(per):
                n = per * i + n
                k, v = (dot(a, w_s[which, n]) for which in (1, 2))
                put_keys(n, k, v, count)
        lax.fori_loop(0, TILES // per, step, None)

    def last_keys(c):
        forward_piece(c).wait_recv()
        if c == 1:
            angles_of(LAST, 0)

        def step(i, _):
            a = a0[LAST, :, slice(*COLS[c])]
            for n in range(PER_LAST):
                n = PER_LAST * i + n
                k, v = (dot(a, w_s[which, n, slice(*COLS[c]), :]) for which in (1, 2))
                if c == 0:
                    kv_s[0, n], kv_s[1, n] = k, v
                else:
                    put_keys(n, kv_s[0, n] + k, kv_s[1, n] + v, 2 * PART)
        lax.fori_loop(0, TILES // PER_LAST, step, None)

    def attend(jobs, count):
        scores = [dot(k0_s[h, :count], q_s[h, :, cols]) for h, cols in jobs]
        weights = []
        for (h, cols), s in zip(jobs, scores):
            old = top_s[h, :, cols]
            top = jnp.maximum(old, s.max(0, keepdims=True))
            top_s[h, :, cols] = top
            weights.append((jnp.exp2((s - top) * SCALE).astype(BF16), jnp.exp2((old - top) * SCALE)))
        for (h, cols), (w, keep) in zip(jobs, weights):
            mix_s[h, :, cols] = mix_s[h, :, cols] * keep + dot(v0_s[h, :, :count], w)

    def between(count, heads):
        def step(p, _):
            attend([(heads * p + h, slice(c, c + 512)) for h in range(heads) for c in range(0, CHIP, 512)], count)
        return step

    def final(own):
        rows = pl.ds(pl.multiple_of(core * OWN if own else (1 - core) * OWN, OWN), OWN)
        attend([(h, rows) for h in range(HEADS)], 2 * PART)
        finish(own)

    half = TILES // 2

    @pl.when(chip == 0)
    def _():
        lax.fori_loop(0, TILES, within, None)
        for own in (False, True):
            finish(own)

    @pl.when(chip == 1)
    def _():
        relay(0)
        lax.fori_loop(0, TILES - 1, within, None)
        relay(1)
        lax.fori_loop(TILES - 1, TILES, within, None)
        keys(0, 2)
        step = between(4 * PART, 2)
        lax.fori_loop(0, half, step, None)
        relay(2)
        lax.fori_loop(half, TILES, step, None)
        keys(2, 3)
        step = between(2 * PART, 4)
        lax.fori_loop(0, 1, step, None)
        relay_piece(0)
        lax.fori_loop(1, 2, step, None)
        relay_piece(1)
        last_keys(0)
        last_keys(1)
        final(False)
        final(True)

    pair.wait_send()
    for p in range(TILES):
        o_copy(p).wait()

    @pl.when(chip == 0)
    def _():
        for j in range(LAST):
            link(j).wait_send()
        for c in range(2):
            link_piece(c).wait_send()

    @pl.when(chip == 1)
    def _():
        for j in range(LAST):
            forward(j).wait_send()
        for c in range(2):
            forward_piece(c).wait_send()


def out_kernel(o_ref, wo_ref, x_ref, y_ref, y_s, y_sem):
    wide = 512

    def y_copy(n):
        cols = pl.ds(pl.multiple_of(n * wide, wide), wide)
        return pltpu.make_async_copy(y_s.at[:, cols], y_ref.at[:, cols], y_sem.at[n])

    def put(n, y):
        cols = pl.ds(pl.multiple_of(n * wide, wide), wide)
        y_s[:, cols] = (x_ref[:, cols].astype(F32) + y).astype(BF16)
        y_copy(n).start()

    for n in range(D // wide):
        put(n, dot(o_ref[...], wo_ref[:, n * wide : (n + 1) * wide]))
    for n in range(D // wide):
        y_copy(n).wait()


def project_out(o, wo, x):
    whole = pl.BlockSpec(memory_space=pltpu.VMEM)
    return pl.pallas_call(
        out_kernel,
        out_shape=jax.ShapeDtypeStruct((OWN, D), BF16),
        in_specs=[whole] * 3,
        out_specs=pl.BlockSpec(memory_space=pltpu.HBM),
        scratch_shapes=[pltpu.VMEM((OWN, D), BF16), pltpu.SemaphoreType.DMA((D // 512,))],
        compiler_params=pltpu.CompilerParams(vmem_limit_bytes=32 * 2**20),
        cost_estimate=pl.CostEstimate(flops=2 * OWN * D * D, bytes_accessed=14 * 2**20, transcendentals=0),
    )(o, wo, x)


def in_hbm(t):
    return pltpu.with_memory_space_constraint(t, pltpu.HBM)


def solution(mesh):
    table = rope_table()

    def step(x, gain, wq, wk, wv, wo):
        hbm = pl.BlockSpec(memory_space=pl.ANY)
        vmem = pltpu.VMEM
        dma = pltpu.SemaphoreType.DMA
        o = pl.pallas_call(
            kernel,
            out_shape=jax.ShapeDtypeStruct((OWN, D), BF16),
            in_specs=[hbm] * 6,
            out_specs=pl.BlockSpec(memory_space=vmem),
            scratch_shapes=[
                vmem((D,), BF16), vmem((OWN, D), BF16), vmem((OWN, D), BF16), vmem((CHIP, D), BF16), vmem((PARTS, 2 * PART, D), BF16),
                vmem((3, TILES, D, TILE), BF16),
                vmem((HEADS, HEAD, CHIP), BF16), vmem((HEADS, CHIP, HEAD), BF16), vmem((HEADS, VROWS, CHIP), BF16),
                vmem((HEADS, MOST, HEAD), BF16), vmem((HEADS, VROWS, MOST), BF16), vmem((OWN, HEAD), F32), vmem((OWN, HEAD), F32),
                vmem((2 * CHIP, HEAD), F32), vmem((HEADS, 1, CHIP), F32), vmem((HEADS, VROWS, CHIP), F32),
                vmem((TILES, OWN, TILE), BF16), vmem((2, TILES, 2 * PART, TILE), F32),
                dma, dma((PARTS,)), dma((3, TILES)), dma, dma, dma, dma((PARTS + 1,)), dma((PARTS + 1,)), dma((PARTS + 1,)), dma((PARTS + 1,)),
                dma((TILES,)), dma((TILES,)),
            ],
            compiler_params=pltpu.CompilerParams(collective_id=0, has_side_effects=True, vmem_limit_bytes=VMEM_LIMIT),
            cost_estimate=pl.CostEstimate(flops=40 * 10**9, bytes_accessed=36 * 2**20, transcendentals=13 * 10**6),
        )(x, in_hbm(gain), wq, wk, wv, in_hbm(jnp.asarray(table)))
        return project_out(o, wo, x)

    tokens, whole = P(("dp", "sp"), None), P(None, None)
    return jax.shard_map(step, mesh=mesh, in_specs=(tokens, P(None), whole, whole, whole, whole), out_specs=tokens, check_vma=False)
```

```python
import functools

import jax
import jax.numpy as jnp
import numpy as np
from jax import lax
from jax.experimental import pallas as pl
from jax.experimental.pallas import tpu as pltpu
from jax.sharding import PartitionSpec as P

HEAD = 128
THETA = 10000
D = 2048
OWN = 512
CHIP = 1024
HEADS = 8
WIDE = HEADS * HEAD
TILE = 256
TILES = WIDE // TILE
PARTS = 4
PART = OWN // PARTS
LAST = PARTS - 1
COLS = ((0, 1024), (1024, 1792), (1792, 2048))
PIECES = len(COLS)
MOST = 2 * 2 * PART
HIDDEN = -2e30
LOG2E = 1.4426950408889634
SCALE = HEAD**-0.5 * LOG2E
VROWS = HEAD + 16
MESH = pl.DeviceIdType.MESH
PER, PER_KEYS, PER_LAST = 2, 2, 4
VMEM_LIMIT = 50 * 2**20
F32, BF16 = jnp.float32, jnp.bfloat16


def rope_table():
    half = HEAD // 2
    place = np.arange(2 * CHIP, dtype=np.float32)[:, None]
    angle = place * np.power(np.float32(THETA), -np.arange(half, dtype=np.float32) / np.float32(half)).astype(np.float32)
    return np.concatenate([np.cos(angle), np.sin(angle)], -1).astype(np.float32)


def dot(a, b, ca=1, cb=0):
    return lax.dot_general(a, b, (((ca,), (cb,)), ((), ())), preferred_element_type=F32)


def kernel(x_ref, gain_hbm, wq_ref, wk_ref, wv_ref, rope_ref, og_ref,
           gain_ref, xs, x0, a_s, a0, w_s, q_s, k_s, v_s, k0_s, v0_s, cos_s, sin_s, rope_s, top_s, mix_s, os_s, kv_s,
           gain_sem, x_sem, w_sem, rope_sem, pair_send, pair_recv, link_send, link_recv, fwd_send, fwd_recv, o_send, o_recv):
    me = lax.axis_index("sp")
    chip, core = lax.div(me, 2), lax.rem(me, 2)
    partner, across = 2 * chip + 1 - core, lax.rem(me + 2, 4)

    barrier = pltpu.get_barrier_semaphore()
    for other in (partner, across):
        pl.semaphore_signal(barrier, inc=1, device_id={"sp": other}, device_id_type=MESH)

    def part(j):
        return pl.ds(j * PART, PART)

    def link(j):
        return pltpu.make_async_remote_copy(src_ref=x_ref.at[part(j)], dst_ref=x0.at[part(j)], send_sem=link_send.at[j],
                                            recv_sem=link_recv.at[j], device_id={"sp": across}, device_id_type=MESH)

    def forward(j):
        rows = a0.at[j, pl.ds(core * PART, PART)]
        return pltpu.make_async_remote_copy(src_ref=rows, dst_ref=rows, send_sem=fwd_send.at[j], recv_sem=fwd_recv.at[j],
                                            device_id={"sp": partner}, device_id_type=MESH)

    def columns(c):
        return pl.ds(COLS[c][0], COLS[c][1] - COLS[c][0])

    def piece(c):
        return a0.at[LAST, pl.ds(core * PART, PART), columns(c)]

    def link_piece(c):
        return pltpu.make_async_remote_copy(
            src_ref=a_s.at[pl.ds(core * OWN + LAST * PART, PART), columns(c)], dst_ref=piece(c), send_sem=link_send.at[LAST + c],
            recv_sem=link_recv.at[LAST + c], device_id={"sp": across}, device_id_type=MESH)

    def forward_piece(c):
        return pltpu.make_async_remote_copy(src_ref=piece(c), dst_ref=piece(c), send_sem=fwd_send.at[LAST + c],
                                            recv_sem=fwd_recv.at[LAST + c], device_id={"sp": partner}, device_id_type=MESH)

    own_rows = pl.ds(core * OWN, OWN)
    pair = pltpu.make_async_remote_copy(src_ref=a_s.at[own_rows], dst_ref=a_s.at[own_rows], send_sem=pair_send, recv_sem=pair_recv,
                                        device_id={"sp": partner}, device_id_type=MESH)
    rope_copy = pltpu.make_async_copy(rope_ref, rope_s, rope_sem)

    def x_copy(j):
        return pltpu.make_async_copy(x_ref.at[part(j)], xs.at[part(j)], x_sem.at[j])

    def w_copy(n, which):
        ref = (wq_ref, wk_ref, wv_ref)[which]
        cols = pl.ds(pl.multiple_of(core * WIDE + n * TILE, TILE), TILE)
        return pltpu.make_async_copy(ref.at[:, cols], w_s.at[which, n], w_sem.at[which, n])

    gain_copy = pltpu.make_async_copy(gain_hbm, gain_ref, gain_sem)
    gain_copy.start()
    for j in range(PARTS):
        x_copy(j).start()
    rope_copy.start()
    for which in range(3):
        w_copy(0, which).start()

    pl.semaphore_wait(barrier, 2)

    @pl.when(chip == 0)
    def _():
        for j in range(LAST):
            link(j).start()

    for n in range(1, TILES):
        for which in range(3):
            w_copy(n, which).start()

    v_s[:, HEAD:, :] = jnp.ones((HEADS, VROWS - HEAD, CHIP), BF16)
    v0_s[:, HEAD:, :] = jnp.ones((HEADS, VROWS - HEAD, MOST), BF16)

    def norm(get, put, count):
        def step(i, _):
            for at in range(0, 64, 16):
                at = pl.multiple_of(i * 64 + at, 16)
                wide = get(at).astype(F32)
                scale = lax.rsqrt(jnp.mean(wide * wide, -1, keepdims=True) + 1e-6)
                put(at, (wide * scale * gain_ref[...].astype(F32)[None]).astype(BF16))
        lax.fori_loop(0, count // 64, step, None)

    def angles(at, rows, to):
        t = rope_s[pl.ds(at, rows), :]
        r = pltpu.roll(t, 64, 1)
        low = lax.broadcasted_iota(jnp.int32, t.shape, 1) < 64
        cos_s[to : to + rows, :] = jnp.where(low, t, r)
        sin_s[to : to + rows, :] = jnp.where(low, -r, t)

    def turn(t, rows):
        t = t.astype(BF16).astype(F32)
        return (t * cos_s[:rows, :] + pltpu.roll(t, 64, 1) * sin_s[:rows, :]).astype(BF16)

    def put_own(at, rows):
        a_s[pl.ds(core * OWN + at, 16), :] = rows

    gain_copy.wait()
    for j in range(PARTS):
        x_copy(j).wait()
    norm(lambda at: xs[pl.ds(at, 16), :], put_own, OWN)
    rope_copy.wait()

    @pl.when(chip == 0)
    def _():
        for c in range(PIECES):
            link_piece(c).start()
    pair.start()

    def project(i, _):
        of = lax.rem(core + lax.div(i, TILES // PER), 2)
        first = lax.rem(i, TILES // PER) * PER
        rows = pl.ds(pl.multiple_of(of * OWN, OWN), OWN)

        @pl.when(i < TILES // PER)
        def _():
            for n in range(PER):
                for which in range(3):
                    w_copy(first + n, which).wait()

        @pl.when(i == TILES // PER)
        def _():
            pair.wait_recv()

        @pl.when(first == 0)
        def _():
            angles(pl.multiple_of(chip * CHIP + of * OWN, OWN), OWN, 0)
        a = a_s[rows, :]
        for n in range(PER):
            n = first + n
            q, k, v = (dot(a, w_s[which, n]) for which in range(3))
            for h in range(2):
                cols = slice(h * HEAD, (h + 1) * HEAD)
                q_s[2 * n + h, :, rows] = turn(q[:, cols], OWN).T
                k_s[2 * n + h, rows, :] = turn(k[:, cols], OWN)
                v_s[2 * n + h, :HEAD, rows] = v[:, cols].astype(BF16).T
    lax.fori_loop(0, 2 * TILES // PER, project, None)

    def relay(j):
        link(j).wait_recv()

        def put(at, rows):
            a0[j, pl.ds(core * PART + at, 16), :] = rows
        norm(lambda at: x0[pl.ds(j * PART + at, 16), :], put, PART)
        forward(j).start()

    def relay_piece(c):
        link_piece(c).wait_recv()
        forward_piece(c).start()

    def within(p, _):
        jobs = [(2 * p + h, b) for h in range(2) for b in range(CHIP // 256)]
        scores = [dot(k_s[h, : (b + 1) * 256, :], q_s[h, :, b * 256 : (b + 1) * 256]) for h, b in jobs]
        ok = lax.broadcasted_iota(jnp.int32, (256, 256), 1) >= lax.broadcasted_iota(jnp.int32, (256, 256), 0)
        weights = []
        for (h, b), s in zip(jobs, scores):
            last = jnp.where(ok, s[b * 256 :], HIDDEN)
            s = jnp.concatenate([s[: b * 256], last], 0) if b else last
            top = s.max(0, keepdims=True)
            top_s[h, :, b * 256 : (b + 1) * 256] = top
            weights.append(jnp.exp2((s - top) * SCALE).astype(BF16))
        for (h, b), p in zip(jobs, weights):
            mix_s[h, :, b * 256 : (b + 1) * 256] = dot(v_s[h, :, : (b + 1) * 256], p)

    def o_cols(p):
        return pl.ds(pl.multiple_of((core * TILES + p) * TILE, TILE), TILE)

    def o_copy(p):
        return pltpu.make_async_remote_copy(src_ref=os_s.at[p], dst_ref=og_ref.at[:, o_cols(p)], send_sem=o_send.at[p],
                                            recv_sem=o_recv.at[p], device_id={"sp": partner}, device_id_type=MESH)

    def finish(own):
        rows = pl.ds(pl.multiple_of(core * OWN if own else (1 - core) * OWN, OWN), OWN)
        for h in range(HEADS):
            o = (mix_s[h, :HEAD, rows] * (1 / mix_s[h, HEAD : HEAD + 1, rows])).astype(BF16).T
            if own:
                og_ref[:, pl.ds(pl.multiple_of(core * WIDE + h * HEAD, HEAD), HEAD)] = o
            else:
                os_s[h // 2, :, h % 2 * HEAD : (h % 2 + 1) * HEAD] = o
                if h % 2:
                    o_copy(h // 2).start()

    def angles_of(j, to):
        for of in range(2):
            angles(of * OWN + j * PART, PART, to + of * PART)

    def put_keys(n, k, v, count):
        for h in range(2):
            cols = slice(h * HEAD, (h + 1) * HEAD)
            k0_s[2 * n + h, :count, :] = turn(k[:, cols], count)
            v0_s[2 * n + h, :HEAD, :count] = v[:, cols].astype(BF16).T

    def keys(first, last):
        count = (last - first) * 2 * PART
        for j in range(first, last):
            forward(j).wait_recv()
            angles_of(j, (j - first) * 2 * PART)
        per = PER_KEYS * 512 // count

        def step(i, _):
            a = a0[first:last].reshape(count, D)
            for n in range(per):
                n = per * i + n
                k, v = (dot(a, w_s[which, n]) for which in (1, 2))
                put_keys(n, k, v, count)
        lax.fori_loop(0, TILES // per, step, None)

    def last_keys(c):
        forward_piece(c).wait_recv()
        if c == PIECES - 1:
            angles_of(LAST, 0)

        def step(i, _):
            a = a0[LAST, :, slice(*COLS[c])]
            for n in range(PER_LAST):
                n = PER_LAST * i + n
                k, v = (dot(a, w_s[which, n, slice(*COLS[c]), :]) for which in (1, 2))
                if c:
                    k, v = kv_s[0, n] + k, kv_s[1, n] + v
                if c < PIECES - 1:
                    kv_s[0, n], kv_s[1, n] = k, v
                else:
                    put_keys(n, k, v, 2 * PART)
        lax.fori_loop(0, TILES // PER_LAST, step, None)

    def attend(jobs, count):
        scores = [dot(k0_s[h, :count], q_s[h, :, cols]) for h, cols in jobs]
        weights = []
        for (h, cols), s in zip(jobs, scores):
            old = top_s[h, :, cols]
            top = jnp.maximum(old, s.max(0, keepdims=True))
            top_s[h, :, cols] = top
            weights.append((jnp.exp2((s - top) * SCALE).astype(BF16), jnp.exp2((old - top) * SCALE)))
        for (h, cols), (w, keep) in zip(jobs, weights):
            mix_s[h, :, cols] = mix_s[h, :, cols] * keep + dot(v0_s[h, :, :count], w)

    def between(count, heads):
        def step(p, _):
            attend([(heads * p + h, slice(c, c + 512)) for h in range(heads) for c in range(0, CHIP, 512)], count)
        return step

    def final(own):
        rows = pl.ds(pl.multiple_of(core * OWN if own else (1 - core) * OWN, OWN), OWN)
        attend([(h, rows) for h in range(HEADS)], 2 * PART)
        finish(own)

    half = TILES // 2

    @pl.when(chip == 0)
    def _():
        lax.fori_loop(0, TILES, within, None)
        for own in (False, True):
            finish(own)

    @pl.when(chip == 1)
    def _():
        relay(0)
        lax.fori_loop(0, TILES - 1, within, None)
        relay(1)
        lax.fori_loop(TILES - 1, TILES, within, None)
        keys(0, 2)
        step = between(4 * PART, 2)
        lax.fori_loop(0, half, step, None)
        relay(2)
        lax.fori_loop(half, TILES, step, None)
        keys(2, 3)
        step = between(2 * PART, 4)
        lax.fori_loop(0, 1, step, None)
        relay_piece(0)
        lax.fori_loop(1, 2, step, None)
        relay_piece(1)
        last_keys(0)
        relay_piece(2)
        last_keys(1)
        last_keys(2)
        final(False)
        final(True)

    pair.wait_send()
    for p in range(TILES):
        o_copy(p).wait()

    @pl.when(chip == 0)
    def _():
        for j in range(LAST):
            link(j).wait_send()
        for c in range(PIECES):
            link_piece(c).wait_send()

    @pl.when(chip == 1)
    def _():
        for j in range(LAST):
            forward(j).wait_send()
        for c in range(PIECES):
            forward_piece(c).wait_send()


def out_kernel(o_ref, wo_ref, x_ref, y_ref, y_s, y_sem):
    wide = 512

    def y_copy(n):
        cols = pl.ds(pl.multiple_of(n * wide, wide), wide)
        return pltpu.make_async_copy(y_s.at[:, cols], y_ref.at[:, cols], y_sem.at[n])

    def put(n, y):
        cols = pl.ds(pl.multiple_of(n * wide, wide), wide)
        y_s[:, cols] = (x_ref[:, cols].astype(F32) + y).astype(BF16)
        y_copy(n).start()

    for n in range(D // wide):
        put(n, dot(o_ref[...], wo_ref[:, n * wide : (n + 1) * wide]))
    for n in range(D // wide):
        y_copy(n).wait()


def project_out(o, wo, x):
    whole = pl.BlockSpec(memory_space=pltpu.VMEM)
    return pl.pallas_call(
        out_kernel,
        out_shape=jax.ShapeDtypeStruct((OWN, D), BF16),
        in_specs=[whole] * 3,
        out_specs=pl.BlockSpec(memory_space=pltpu.HBM),
        scratch_shapes=[pltpu.VMEM((OWN, D), BF16), pltpu.SemaphoreType.DMA((D // 512,))],
        compiler_params=pltpu.CompilerParams(vmem_limit_bytes=32 * 2**20),
        cost_estimate=pl.CostEstimate(flops=2 * OWN * D * D, bytes_accessed=14 * 2**20, transcendentals=0),
    )(o, wo, x)


def in_hbm(t):
    return pltpu.with_memory_space_constraint(t, pltpu.HBM)


def solution(mesh):
    table = rope_table()

    def step(x, gain, wq, wk, wv, wo):
        hbm = pl.BlockSpec(memory_space=pl.ANY)
        vmem = pltpu.VMEM
        dma = pltpu.SemaphoreType.DMA
        o = pl.pallas_call(
            kernel,
            out_shape=jax.ShapeDtypeStruct((OWN, D), BF16),
            in_specs=[hbm] * 6,
            out_specs=pl.BlockSpec(memory_space=vmem),
            scratch_shapes=[
                vmem((D,), BF16), vmem((OWN, D), BF16), vmem((OWN, D), BF16), vmem((CHIP, D), BF16), vmem((PARTS, 2 * PART, D), BF16),
                vmem((3, TILES, D, TILE), BF16),
                vmem((HEADS, HEAD, CHIP), BF16), vmem((HEADS, CHIP, HEAD), BF16), vmem((HEADS, VROWS, CHIP), BF16),
                vmem((HEADS, MOST, HEAD), BF16), vmem((HEADS, VROWS, MOST), BF16), vmem((OWN, HEAD), F32), vmem((OWN, HEAD), F32),
                vmem((2 * CHIP, HEAD), F32), vmem((HEADS, 1, CHIP), F32), vmem((HEADS, VROWS, CHIP), F32),
                vmem((TILES, OWN, TILE), BF16), vmem((2, TILES, 2 * PART, TILE), F32),
                dma, dma((PARTS,)), dma((3, TILES)), dma, dma, dma, dma((LAST + PIECES,)), dma((LAST + PIECES,)), dma((LAST + PIECES,)), dma((LAST + PIECES,)),
                dma((TILES,)), dma((TILES,)),
            ],
            compiler_params=pltpu.CompilerParams(collective_id=0, has_side_effects=True, vmem_limit_bytes=VMEM_LIMIT),
            cost_estimate=pl.CostEstimate(flops=40 * 10**9, bytes_accessed=36 * 2**20, transcendentals=13 * 10**6),
        )(x, in_hbm(gain), wq, wk, wv, in_hbm(jnp.asarray(table)))
        return project_out(o, wo, x)

    tokens, whole = P(("dp", "sp"), None), P(None, None)
    return jax.shard_map(step, mesh=mesh, in_specs=(tokens, P(None), whole, whole, whole, whole), out_specs=tokens, check_vma=False)
```
